32 devices in a mesh: rep: 4 (over y, core), shard: 8 (over z, x).
Axes of the slice: x: 2, y: 2, z: 4, core: 2. Of those that a mesh axis runs over, the one named last changes fastest.
Arguments:
- hidden: bfloat16 [14336, 3584], P(('rep', 'shard')), may hold values from -144 to 144
- cotangent: bfloat16 [14336, 1024], P(('rep', 'shard')), may hold values from -6 to 6
- seq_ids: int32 [32, 448], P(('rep', 'shard')), may hold values from 0 to 3, as said below
- response_mask: int32 [32, 448], P(('rep', 'shard')), may hold values from 0 to 1, as said below
- group_ids: int32 [32, 4], P(('rep', 'shard')), may hold values from 0 to 15
- rewards: float32 [32, 4], P(('rep', 'shard')), may hold values from -6 to 6
- new_logp: float32 [32, 448], P(('rep', 'shard')), may hold values from -1.5 to -0.1
- old_logp: float32 [32, 448], P(('rep', 'shard')), may hold values from -1.5 to -0.1
- ref_logp: float32 [32, 448], P(('rep', 'shard')), may hold values from -1.5 to -0.1
- master: float32 [3, 3584, 1024], P(None, 'shard'), may hold values from -6 to 6
Outputs:
- new_master: float32 [3584, 1024], P('shard')
- rollout: bfloat16 [3, 3584, 2048], P(None, None, 'shard')
The draws below stay inside these ranges and needn't reach their ends.
Inputs may be any that keep to these rules, and one draw needn't show every extreme that they name: `seq_ids`: each row numbers its device's 4 sequences in token order, never falling, each with one token or more. `response_mask`: within a sequence, prompt tokens come before response tokens; a sequence may have no response tokens.
All inputs are finite; a program needn't handle non-finite values.
Results may differ from the reference program's by a relative error of at most 0.0095.
Values may be sent and summed in bfloat16 or wider, within the bound.
A program may use at most 128 MiB of HBM per device.

```python
import jax
import jax.numpy as jnp
from jax import lax

D = 3584
HEAD = 128
KV_HEADS = 4
KV = 1024
TP = 8
LAYERS = 3
TOK_DEV = 448
SEQ_DEV = 4
TOKENS = 14336
GROUPS = 16
COPIES = 1
DEVICES = 32


def draw_hidden(key, part):
    column = jnp.arange(D, dtype=jnp.int32).astype(jnp.float32) / (D - 1)
    noise_key = jax.random.fold_in(key, 21)
    base = jnp.clip(jax.random.normal(noise_key, (TOKENS, D), jnp.float32), -6.0, 6.0)
    scale = 1.0 + 5.0 * column
    paired = jax.random.permutation(jax.random.fold_in(key, 22), DEVICES).astype(jnp.int32)
    row_block = jnp.arange(TOKENS, dtype=jnp.int32) // TOK_DEV
    col_block = jnp.arange(D, dtype=jnp.int32) // (D // DEVICES)
    target = paired[row_block]
    spike = jnp.where(target[:, None] == col_block[None, :], 4.0, 1.0)
    return (base * scale[None, :] * spike).astype(jnp.bfloat16)


def sequence_layout(key):
    row_keys = jax.random.split(jax.random.fold_in(key, 11), DEVICES)

    def row_bounds(row_key):
        picked = jax.random.permutation(row_key, TOK_DEV - 1)[:SEQ_DEV - 1] + 1
        return jnp.sort(picked).astype(jnp.int32)
    boundaries = jax.vmap(row_bounds)(row_keys)
    positions = jnp.arange(TOK_DEV, dtype=jnp.int32)
    seq_index = jnp.sum((positions[None, :, None] >= boundaries[:, None, :]).astype(jnp.int32), axis=2).astype(jnp.int32)
    starts = jnp.concatenate([jnp.zeros((DEVICES, 1), jnp.int32), boundaries], axis=1)
    finish = jnp.concatenate([boundaries, jnp.full((DEVICES, 1), TOK_DEV, jnp.int32)], axis=1)
    seq_lengths = finish - starts
    prompt = jax.random.randint(jax.random.fold_in(key, 12), (DEVICES, SEQ_DEV), 0, seq_lengths // 2 + 1).astype(jnp.int32)
    no_reply = jax.random.randint(jax.random.fold_in(key, 13), (DEVICES, SEQ_DEV), 0, 8) == 0
    prompt = jnp.where(no_reply, seq_lengths, prompt)
    tok_start = jnp.take_along_axis(starts, seq_index, axis=1)
    tok_prompt = jnp.take_along_axis(prompt, seq_index, axis=1)
    reply_mask = (positions[None, :] - tok_start >= tok_prompt).astype(jnp.int32)
    return (seq_index, reply_mask)


def draw_seq_ids(key, part):
    return sequence_layout(key)[0]


def draw_response_mask(key, part):
    return sequence_layout(key)[1]


def touch_ends(array, rng, low, largest):
    longest = array.shape.index(max(array.shape))
    spots = []
    for shift in (0, 1):
        where = [jax.random.randint(jax.random.fold_in(rng, axis), (), 0, length) for axis, length in enumerate(array.shape)]
        where[longest] = (where[longest] + shift) % array.shape[longest]
        spots.append(tuple(where))
    return array.at[spots[0]].set(low).at[spots[1]].set(largest)


def steps_of(own_key, dims, pieces, least, top_value):
    level, own = 1.0, jax.random.fold_in(own_key, 6)
    for position, blocks in pieces:
        heights = jnp.exp(jax.random.uniform(jax.random.fold_in(own, position), (blocks,), jnp.float32, least / len(pieces), top_value / len(pieces)))
        level = level * jnp.repeat(heights, dims[position] // blocks).reshape([-1 if axis == position else 1 for axis in range(len(dims))])
    return level


def gaussian(stream_key, shape, scale, reach, shards=(), held_as=jnp.bfloat16):
    level = steps_of(stream_key, shape, shards, -0.22, 0.18) if shards else 1.0
    values = jax.random.normal(stream_key, shape, jnp.float32) * scale * level
    return jnp.minimum(jnp.maximum(values, -reach), reach).astype(held_as)


def setup_inputs(seed: int = 0) -> dict:
    arg_keys = jax.random.split(jax.random.key(seed), 11)
    hidden = draw_hidden(jax.random.fold_in(arg_keys[10], 71), 0)
    cotangent = gaussian(arg_keys[1], (TOKENS, KV), 1.0, 6.0, ((0, 32),))
    seq_ids = draw_seq_ids(jax.random.fold_in(arg_keys[10], 71), 0)
    response_mask = draw_response_mask(jax.random.fold_in(arg_keys[10], 71), 0)
    group_ids = touch_ends(jax.random.randint(arg_keys[4], (DEVICES, SEQ_DEV), 0, GROUPS), jax.random.fold_in(arg_keys[4], 1), 0, GROUPS - 1).astype(jnp.int32)
    rewards = gaussian(arg_keys[5], (DEVICES, SEQ_DEV), 1.0, 6.0, ((0, 32),), jnp.float32)
    new_logp = jnp.clip(-1.5 + 1.4 * jax.random.uniform(arg_keys[6], (DEVICES, TOK_DEV), jnp.float32) ** steps_of(arg_keys[6], (DEVICES, TOK_DEV), ((0, 32),), -0.2, 0.2), -1.5, -0.1)
    old_logp = jnp.clip(-1.5 + 1.4 * jax.random.uniform(arg_keys[7], (DEVICES, TOK_DEV), jnp.float32) ** steps_of(arg_keys[7], (DEVICES, TOK_DEV), ((0, 32),), -0.2, 0.2), -1.5, -0.1)
    ref_logp = jnp.clip(-1.5 + 1.4 * jax.random.uniform(arg_keys[8], (DEVICES, TOK_DEV), jnp.float32) ** steps_of(arg_keys[8], (DEVICES, TOK_DEV), ((0, 32),), -0.2, 0.2), -1.5, -0.1)
    master = gaussian(arg_keys[9], (LAYERS, D, KV), 1.0, 6.0, ((1, 8),), jnp.float32)
    return dict(hidden=hidden, cotangent=cotangent, seq_ids=seq_ids, response_mask=response_mask, group_ids=group_ids, rewards=rewards, new_logp=new_logp, old_logp=old_logp, ref_logp=ref_logp, master=master)


def token_coef(seq_row, mask_row, adv_row, new_row, old_row, ref_row):
    onehot = (seq_row[:, None] == jnp.arange(SEQ_DEV, dtype=jnp.int32)[None, :]).astype(jnp.float32)
    maskf = mask_row.astype(jnp.float32)
    lengths = jnp.maximum(jnp.dot(maskf, onehot, precision=lax.Precision.HIGHEST), 1.0)
    tok_len = jnp.dot(onehot, lengths, precision=lax.Precision.HIGHEST)
    tok_adv = jnp.dot(onehot, adv_row, precision=lax.Precision.HIGHEST)
    surrogate = -tok_adv * jnp.exp(new_row - old_row) + 0.2 * (1.0 - jnp.exp(ref_row - new_row))
    return maskf / tok_len * surrogate

def group_advantage(group_flat, reward_flat, stats):
    groups = stats.shape[1]
    onehot = (group_flat[:, None] == jnp.arange(groups, dtype=jnp.int32)[None, :]).astype(jnp.float32)
    count = jnp.maximum(stats[0], 1.0)
    mean = stats[1] / count
    spread = jnp.sqrt(jnp.maximum(stats[2] / count - mean * mean, 0.0))
    tok_mean = jnp.dot(onehot, mean, precision=lax.Precision.HIGHEST)
    tok_std = jnp.dot(onehot, jnp.maximum(spread, 0.5), precision=lax.Precision.HIGHEST)
    return (reward_flat - tok_mean) / tok_std

def group_sums(group_flat, reward_flat, groups):
    onehot = (group_flat[:, None] == jnp.arange(groups, dtype=jnp.int32)[None, :]).astype(jnp.float32)
    values = jnp.stack([jnp.ones_like(reward_flat), reward_flat, reward_flat * reward_flat], axis=0)
    return jnp.dot(values, onehot, precision=lax.Precision.HIGHEST)

def device_gradient(hidden, delta):
    hidden_rows = hidden.reshape(DEVICES, TOK_DEV, D)
    delta_rows = delta.reshape(DEVICES, TOK_DEV, KV)

    def add_device(running, pair):
        term = lax.dot_general(pair[0], pair[1], (((0,), (0,)), ((), ())), preferred_element_type=jnp.float32)
        partial_value = lax.optimization_barrier(term.astype(jnp.bfloat16))
        return (running + partial_value.astype(jnp.float32), None)
    grad, _ = lax.scan(add_device, jnp.zeros((D, KV), jnp.float32), (hidden_rows, delta_rows))
    return grad

def rollout_layout(layers):
    paired = layers.reshape(LAYERS, D, 2, KV_HEADS, HEAD).transpose(0, 1, 3, 2, 4)
    paired = paired.reshape(LAYERS, D, KV_HEADS, 2 * HEAD)
    by_rank = jnp.repeat(paired, TP // KV_HEADS, axis=2)
    copies = jnp.tile(by_rank, (1, 1, COPIES, 1))
    return copies.reshape(LAYERS, D, COPIES * TP * 2 * HEAD)

def reference(hidden, cotangent, seq_ids, response_mask, group_ids, rewards, new_logp, old_logp, ref_logp, master):
    group_flat = group_ids.reshape(-1)
    reward_flat = rewards.reshape(-1)
    stats = group_sums(group_flat, reward_flat, GROUPS)
    advantage = group_advantage(group_flat, reward_flat, stats).reshape(rewards.shape)
    coef = jax.vmap(token_coef)(seq_ids, response_mask, advantage, new_logp, old_logp, ref_logp)
    delta = (coef.reshape(-1)[:, None] * cotangent.astype(jnp.float32)).astype(jnp.bfloat16)
    grad = device_gradient(hidden, delta)
    rms = jnp.sqrt(jnp.sum(grad * grad) / (D * KV) + 1e-06)
    new_master = master[0] - 0.5 * grad / rms
    layers = jnp.concatenate([new_master[None], master[1:]], axis=0).astype(jnp.bfloat16)
    rollout = rollout_layout(layers)
    return (new_master, rollout)
```

```python
import functools

import jax
import jax.numpy as jnp
from jax import lax
from jax.experimental import pallas as pl
from jax.experimental.pallas import tpu as pltpu
from jax.sharding import PartitionSpec as P

HEAD = 128
KV_HEADS = 4
TP = 8
SEQ_DEV = 4
WIDE = 2 * HEAD
LANES = 128
SUB = 16
TILE = 256
MESH = pl.DeviceIdType.MESH


def token_terms(seq_row, mask_row, new_row, old_row, ref_row):
    onehot = (seq_row[:, None] == jnp.arange(SEQ_DEV, dtype=jnp.int32)[None, :]).astype(jnp.float32)
    maskf = mask_row.astype(jnp.float32)
    lengths = jnp.maximum(jnp.sum(maskf[:, None] * onehot, axis=0), 1.0)
    tok_len = jnp.sum(onehot * lengths[None, :], axis=1)
    weight = maskf / tok_len
    ratio = -weight * jnp.exp(new_row - old_row)
    fixed = weight * (0.2 * (1.0 - jnp.exp(ref_row - new_row)))
    return jnp.concatenate(
        [onehot * ratio[:, None], fixed[:, None], jnp.zeros((onehot.shape[0], 3), jnp.float32)], axis=1
    )


def flip(index, bit):
    step = 1 << bit
    here = (index // step) % 2
    return index + (1 - 2 * here) * step, here


def exchange_kernel(
    n_rep, n_shard, split, group_ref, reward_ref, token_ref, hidden_ref, cot_ref, master_ref,
    mb_ref, gb_out, nm_out, scale_ref,
    part, sums, zin, grad, rows_in, delta, stage_in, stage_out,
    small, small_in, send_sems, recv_sems, local_sems,
):
    z_count = n_shard // 2
    rep_bits = n_rep.bit_length() - 1
    dims = rep_bits
    r, s = lax.axis_index("rep"), lax.axis_index("shard")
    core, x, zi = r % 2, s % 2, s // 2
    head = zi % KV_HEADS
    first = zi - head
    features, toks = hidden_ref.shape[1], hidden_ref.shape[0]
    layer_count, rows = master_ref.shape[0], master_ref.shape[1]
    sub = rows // split
    counter = [0]
    started = []

    def send(src, dst, device):
        number = counter[0]
        counter[0] += 1
        copy = pltpu.make_async_remote_copy(
            src_ref=src, dst_ref=dst, send_sem=send_sems.at[number], recv_sem=recv_sems.at[number],
            device_id=device, device_id_type=MESH,
        )
        copy.start()
        started.append(copy)
        return copy

    def local(src, dst, number):
        copy = pltpu.make_async_copy(src, dst, local_sems.at[number])
        copy.start()
        return copy

    mate = (flip(r, 0)[0], s)
    options = []
    for bit in range(1, rep_bits):
        other, here = flip(r, bit)
        options.append((other, s, here))
    other, here = flip(s, 0)
    options.append((r, other, here))
    partners, bits = [], []
    for i in range(dims):
        a, b = options[i], options[(i + 1) % dims]
        partners.append(tuple(a[k] + core * (b[k] - a[k]) for k in range(2)))
        bits.append(a[2] + core * (b[2] - a[2]))
    z_peers = [None] + [(r, ((zi + d) % z_count) * 2 + x) for d in range(1, z_count)]
    tp_zi = [first + (head + d) % KV_HEADS for d in range(KV_HEADS)]
    tp_peers = [(r, tp_zi[d] * 2 + x) for d in range(KV_HEADS)]

    quarter = r % split
    fetch = local(master_ref.at[:, pl.ds(pl.multiple_of(quarter * sub, SUB), sub), :], stage_in, 0)

    barrier = pltpu.get_barrier_semaphore()
    everyone = [mate] + [o[:2] for o in options] + z_peers[1:]
    for device in everyone:
        pl.semaphore_signal(barrier, inc=1, device_id=device, device_id_type=MESH)

    hot, reward = group_ref[...], reward_ref[...]
    small[0] = jnp.concatenate(
        [jnp.sum(hot, axis=0, keepdims=True), jnp.sum(hot * reward, axis=0, keepdims=True),
         jnp.sum(hot * (reward * reward), axis=0, keepdims=True),
         jnp.zeros((5, hot.shape[1]), jnp.float32)], axis=0)
    pl.semaphore_wait(barrier, len(everyone))

    stat_copies = [send(small.at[0], small_in.at[d - 1], z_peers[d]) for d in range(1, z_count)]

    fetch.wait()
    for h in range(KV_HEADS):
        for l in range(layer_count):
            stage_out[h, l, :, :HEAD] = stage_in[l, :, h * HEAD:(h + 1) * HEAD].astype(jnp.bfloat16)
            low = KV_HEADS * HEAD + h * HEAD
            stage_out[h, l, :, HEAD:] = stage_in[l, :, low:low + HEAD].astype(jnp.bfloat16)
    yi = quarter // 2
    for copy in stat_copies:
        copy.wait_recv()
    slot = z_count - 1
    total = small[0]
    for d in range(1, z_count):
        total = total + small_in[d - 1]
    small[1] = total
    level = 1
    for k, device in enumerate([mate] + partners):
        copy = send(small.at[level], small_in.at[slot], device)
        if k == 0:
            own_copy = local(stage_out.at[head], mb_ref.at[core, x, yi, zi], 1)
            m1 = [send(stage_out.at[(head + d) % KV_HEADS], mb_ref.at[core, x, yi, zi], z_peers[d])
                  for d in range(1, z_count)]
        copy.wait_recv()
        total = total + small_in[slot]
        slot += 1
        level += 1
        small[level] = total

    count = jnp.maximum(total[0:1], 1.0)
    mean = total[1:2] / count
    spread = jnp.maximum(jnp.sqrt(jnp.maximum(total[2:3] / count - mean * mean, 0.0)), 0.5)
    own_mean = jnp.sum(hot * mean, axis=1, keepdims=True)
    own_std = jnp.sum(hot * spread, axis=1, keepdims=True)
    own_std = jnp.where(own_std > 0.0, own_std, 1.0)
    advantage = (reward[:, 0:1] - own_mean) / own_std
    coef = token_ref[:, SEQ_DEV:SEQ_DEV + 1]
    for j in range(SEQ_DEV):
        coef = coef + token_ref[:, j:j + 1] * advantage[j:j + 1, :]
    for h in range(KV_HEADS):
        for side in range(2):
            low = side * KV_HEADS * HEAD + h * HEAD
            at = h * WIDE + side * HEAD
            delta[:, at:at + HEAD] = (coef * cot_ref[:, low:low + HEAD].astype(jnp.float32)).astype(jnp.bfloat16)

    half = features // 2

    def multiply(base):
        @pl.loop(0, half // TILE)
        def _(i):
            at = pl.multiple_of(base + i * TILE, TILE)
            out = lax.dot_general(
                hidden_ref[:, pl.ds(at, TILE)], delta[...], (((0,), (0,)), ((), ())),
                preferred_element_type=jnp.float32,
            ).astype(jnp.bfloat16)
            for h in range(KV_HEADS):
                part[h, pl.ds(at, TILE), :] = out[:, h * WIDE:(h + 1) * WIDE]

    offsets, lens = [core * half], [half]
    for i in range(dims):
        lens.append(lens[-1] // 2)
        offsets.append(offsets[-1] + bits[i] * lens[-1])
    starts, at = [], 0
    for length in lens:
        starts.append(at)
        at += length
    order = [(head + k + 1) % KV_HEADS for k in range(KV_HEADS)]

    away = (1 - core) * half
    multiply(away)
    inbound = {}
    for k in range(KV_HEADS):
        inbound[0, k] = send(
            part.at[order[k], pl.ds(pl.multiple_of(away, SUB), half)],
            sums.at[order[k], pl.ds(starts[0], half)], mate)
    multiply(core * half)

    own_copy.wait()
    for copy in m1:
        copy.wait_recv()
    xy = [(r, flip(s, 0)[0])]
    first_at = (1 - x, yi)
    if split == 4:
        other = flip(r, 1)[0]
        xy = [(r + core * (other - r), s + (1 - core) * (1 - 2 * x)),
              (r + (1 - core) * (other - r), s + core * (1 - 2 * x))]
        first_at = (x + (1 - core) * (1 - 2 * x), yi + core * (1 - 2 * yi))
    own_block = mb_ref.at[core, x, yi]
    spread_copies = [send(own_block, own_block, device) for device in xy]
    forward = []

    inner = min(lens[-1], 112)

    def add_in(i, h):
        base = offsets[i]

        @pl.loop(0, lens[i] // inner)
        def _(t):
            at = pl.multiple_of(base + t * inner, SUB)
            from_at = pl.multiple_of(starts[i] + t * inner, SUB)
            part[h, pl.ds(at, inner), :] = (
                part[h, pl.ds(at, inner), :].astype(jnp.float32)
                + sums[h, pl.ds(from_at, inner), :].astype(jnp.float32)
            ).astype(jnp.bfloat16)

    z_copies = []
    for t in range(KV_HEADS + dims):
        for i in range(dims + 1):
            k = t - i
            if k < 0 or k >= KV_HEADS:
                continue
            inbound[i, k].wait_recv()
            add_in(i, order[k])
            if i < dims:
                gone = offsets[i] + (1 - bits[i]) * lens[i + 1]
                inbound[i + 1, k] = send(
                    part.at[order[k], pl.ds(pl.multiple_of(gone, SUB), lens[i + 1])],
                    sums.at[order[k], pl.ds(starts[i + 1], lens[i + 1])], partners[i])
            else:
                for d in range(1, z_count):
                    if d % KV_HEADS == (k + 1) % KV_HEADS:
                        z_copies.append(send(
                            part.at[order[k], pl.ds(pl.multiple_of(offsets[-1], SUB), lens[-1])],
                            zin.at[d - 1], z_peers[d]))
        if t == 2 and split == 4:
            spread_copies[0].wait_recv()
            block = mb_ref.at[core, first_at[0], first_at[1]]
            forward.append(send(block, block, xy[1]))

    for copy in z_copies:
        copy.wait_recv()
    base = offsets[-1]

    def gather_sum(t, acc):
        at = pl.multiple_of(base + t * inner, SUB)
        g = part[head, pl.ds(at, inner), :].astype(jnp.float32)
        for d in range(1, z_count):
            g = g + zin[d - 1, pl.ds(pl.multiple_of(t * inner, SUB), inner), :].astype(jnp.float32)
        grad[pl.ds(at, inner), :] = g.astype(jnp.bfloat16)
        return acc + jnp.sum(g * g, axis=0, keepdims=True)

    squares = lax.fori_loop(0, lens[-1] // inner, gather_sum, jnp.zeros((1, WIDE), jnp.float32))
    square = jnp.broadcast_to(jnp.sum(squares, axis=1, keepdims=True), small.shape[1:])
    level += 1
    small[level] = square
    square_copies = []
    for d in range(1, KV_HEADS):
        square_copies.append(send(small.at[level], small_in.at[slot], tp_peers[d]))
        slot += 1
    slot_base = slot - (KV_HEADS - 1)

    for step, i in enumerate(list(reversed(range(dims))) + [-1]):
        device = mate if i < 0 else partners[i]
        span = pl.ds(pl.multiple_of(offsets[i + 1], SUB), lens[i + 1])
        copy = send(grad.at[span], grad.at[span], device)
        if step == 0:
            for other in square_copies:
                other.wait_recv()
            for d in range(KV_HEADS - 1):
                square = square + small_in[slot_base + d]
        level += 1
        small[level] = square
        square_copy = send(small.at[level], small_in.at[slot], device)
        square_copy.wait_recv()
        square = square + small_in[slot]
        slot += 1
        copy.wait_recv()

    piece = rows // 2
    nm_copies = []
    mine = pl.ds(pl.multiple_of(core * piece, SUB), piece)
    for d in range(1, KV_HEADS):
        at = pl.multiple_of((tp_zi[d] * 2 + x) * rows + core * piece, SUB)
        nm_copies.append(send(grad.at[pl.ds(at, piece)], rows_in.at[head, mine], tp_peers[d]))

    for copy in spread_copies[len(spread_copies) - 1:] + forward:
        copy.wait_recv()
    last = send(mb_ref.at[core], mb_ref.at[core], mate)

    rms = jnp.sqrt(square / (features * KV_HEADS * WIDE) + 1e-06)
    scale_ref[...] = 0.5 / rms[:, :LANES]
    done = [local(grad, gb_out, 0)]
    done.append(local(grad.at[pl.ds(pl.multiple_of(s * rows, SUB), rows)], nm_out.at[head], 1))
    passed = []
    for d in range(1, KV_HEADS):
        nm_copies[d - 1].wait_recv()
        source = (head + KV_HEADS - d) % KV_HEADS
        passed.append(send(rows_in.at[source, mine], rows_in.at[source, mine], mate))
    for d in range(1, KV_HEADS):
        passed[d - 1].wait_recv()
        source = (head + KV_HEADS - d) % KV_HEADS
        done.append(local(rows_in.at[source], nm_out.at[source], d + 1))
    last.wait_recv()
    for copy in done:
        copy.wait()
    for copy in started:
        copy.wait_send()


def finish_kernel(mb_ref, gb_ref, nm_ref, scale_ref, master_ref, new_ref, out_ref):
    scale = scale_ref[0:1, 0:1]
    for h in range(KV_HEADS):
        for side in range(2):
            low = side * KV_HEADS * HEAD + h * HEAD
            new_ref[:, low:low + HEAD] = (
                master_ref[0, :, low:low + HEAD]
                - scale * nm_ref[h, :, side * HEAD:(side + 1) * HEAD].astype(jnp.float32))
    _, _, y_count, z_count, layer_count, sub, _ = mb_ref.shape
    for z in range(z_count):
        for x in range(2):
            for y in range(y_count):
                for c in range(2):
                    at = (((z * 2 + x) * y_count + y) * 2 + c) * sub
                    span = slice(at, at + sub)
                    out_ref[0, span, :] = (
                        mb_ref[c, x, y, z, 0].astype(jnp.float32)
                        - scale * gb_ref[span, :].astype(jnp.float32)).astype(jnp.bfloat16)
                    for l in range(1, layer_count):
                        out_ref[l, span, :] = mb_ref[c, x, y, z, l]


def per_device(
    n_rep, n_shard, hidden, cotangent, seq_ids, response_mask, group_ids, rewards, new_logp, old_logp, ref_logp,
    master,
):
    groups = n_rep * n_shard * SEQ_DEV // 8
    wide = -(-groups // LANES) * LANES
    toks, features = hidden.shape
    layer_count, rows, cols = master.shape
    z_count = n_shard // 2
    split = 4 if n_rep % 4 == 0 and (rows // 4) % SUB == 0 else 2
    sub = rows // split
    dims = n_rep.bit_length() - 1
    final = features // 2 ** (dims + 1)
    hot = (group_ids[0][:, None] == jnp.arange(wide, dtype=jnp.int32)[None, :]).astype(jnp.float32)
    hot = jnp.pad(hot, ((0, 8 - SEQ_DEV), (0, 0)))
    reward = jnp.broadcast_to(jnp.pad(rewards[0], (0, 8 - SEQ_DEV))[:, None], (8, wide))
    terms = token_terms(seq_ids[0], response_mask[0], new_logp[0], old_logp[0], ref_logp[0])
    bf16, f32 = jnp.bfloat16, jnp.float32
    vmem, hbm = pl.BlockSpec(memory_space=pltpu.VMEM), pl.BlockSpec(memory_space=pl.ANY)
    mb_shape = (2, 2, split // 2, z_count, layer_count, sub, WIDE)
    sem_count = 64 + 4 * z_count
    landing = features // 2 * 2
    mb, gb, nm, scale = pl.pallas_call(
        functools.partial(exchange_kernel, n_rep, n_shard, split),
        out_shape=(
            jax.ShapeDtypeStruct(mb_shape, bf16),
            jax.ShapeDtypeStruct((features, WIDE), bf16),
            jax.ShapeDtypeStruct((KV_HEADS, rows, WIDE), bf16),
            jax.ShapeDtypeStruct((8, LANES), f32),
        ),
        in_specs=[vmem] * 5 + [hbm],
        out_specs=(hbm, hbm, hbm, vmem),
        scratch_shapes=[
            pltpu.VMEM((KV_HEADS, features, WIDE), bf16),
            pltpu.VMEM((KV_HEADS, landing, WIDE), bf16),
            pltpu.VMEM((z_count - 1, final, WIDE), bf16),
            pltpu.VMEM((features, WIDE), bf16),
            pltpu.VMEM((KV_HEADS, rows, WIDE), bf16),
            pltpu.VMEM((toks, cols), bf16),
            pltpu.VMEM((layer_count, sub, cols), f32),
            pltpu.VMEM((KV_HEADS, layer_count, sub, WIDE), bf16),
            pltpu.VMEM((2 * dims + 6, 8, wide), f32),
            pltpu.VMEM((z_count + 2 * dims + 6, 8, wide), f32),
            pltpu.SemaphoreType.DMA((sem_count,)),
            pltpu.SemaphoreType.DMA((sem_count,)),
            pltpu.SemaphoreType.DMA((8,)),
        ],
        compiler_params=pltpu.CompilerParams(
            collective_id=0, has_side_effects=True, vmem_limit_bytes=56 * 2**20
        ),
        name="exchange",
    )(hot, reward, terms, hidden, cotangent, master)
    steps = KV_HEADS
    new_master, rollout = pl.pallas_call(
        finish_kernel,
        grid=(steps,),
        out_shape=(
            jax.ShapeDtypeStruct((rows, cols), f32),
            jax.ShapeDtypeStruct((layer_count, features, WIDE), bf16),
        ),
        in_specs=[
            pl.BlockSpec((2, 2, split // 2, z_count // steps, layer_count, sub, WIDE),
                         lambda i: (0, 0, 0, i, 0, 0, 0)),
            pl.BlockSpec((features // steps, WIDE), lambda i: (i, 0)),
            pl.BlockSpec((KV_HEADS, rows // steps, WIDE), lambda i: (0, i, 0)),
            pl.BlockSpec((8, LANES), lambda i: (0, 0)),
            pl.BlockSpec((1, rows // steps, cols), lambda i: (0, i, 0)),
        ],
        out_specs=(
            pl.BlockSpec((rows // steps, cols), lambda i: (i, 0)),
            pl.BlockSpec((layer_count, features // steps, WIDE), lambda i: (0, i, 0)),
        ),
        name="finish",
    )(mb, gb, nm, scale, master)
    return (new_master, rollout)


def solution(mesh):
    tokens = P(("rep", "shard"), None)
    return jax.shard_map(
        functools.partial(per_device, mesh.shape["rep"], mesh.shape["shard"]),
        mesh=mesh,
        in_specs=(tokens,) * 9 + (P(None, "shard", None),),
        out_specs=(P("shard", None), P(None, None, "shard")),
        check_vma=False,
    )
```

```python
import functools

import jax
import jax.numpy as jnp
from jax import lax
from jax.experimental import pallas as pl
from jax.experimental.pallas import tpu as pltpu
from jax.sharding import PartitionSpec as P

HEAD = 128
KV_HEADS = 4
TP = 8
SEQ_DEV = 4
WIDE = 2 * HEAD
LANES = 128
SUB = 16
TILE = 256
MESH = pl.DeviceIdType.MESH


def token_rows(seq_row, mask_row, new_row, old_row, ref_row):
    maskf = mask_row.astype(jnp.float32)
    onehot = [(seq_row == j).astype(jnp.float32) for j in range(SEQ_DEV)]
    tok_len = jnp.zeros_like(maskf)
    for hot in onehot:
        tok_len = tok_len + hot * jnp.maximum(jnp.sum(maskf * hot, axis=1, keepdims=True), 1.0)
    weight = maskf / tok_len
    ratio = -weight * jnp.exp(new_row - old_row)
    return [hot * ratio for hot in onehot] + [weight * (0.2 * (1.0 - jnp.exp(ref_row - new_row)))]


def flip(index, bit):
    step = 1 << bit
    here = (index // step) % 2
    return index + (1 - 2 * here) * step, here


def exchange_kernel(
    n_rep, n_shard, split, group_ref, reward_ref, seq_ref, mask_ref, new_ref, old_ref, ref_ref,
    hidden_ref, cot_ref, master_ref,
    mb_ref, gb_out, nm_out, scale_ref,
    part, sums, zin, grad, rows_in, delta, stage_in, stage_out,
    small, small_in, token_t, send_sems, recv_sems, local_sems,
):
    z_count = n_shard // 2
    rep_bits = n_rep.bit_length() - 1
    dims = rep_bits
    r, s = lax.axis_index("rep"), lax.axis_index("shard")
    core, x, zi = r % 2, s % 2, s // 2
    head = zi % KV_HEADS
    first = zi - head
    features, toks = hidden_ref.shape[1], hidden_ref.shape[0]
    layer_count, rows = master_ref.shape[0], master_ref.shape[1]
    sub = rows // split
    counter = [0]
    started = []

    def send(src, dst, device):
        number = counter[0]
        counter[0] += 1
        copy = pltpu.make_async_remote_copy(
            src_ref=src, dst_ref=dst, send_sem=send_sems.at[number], recv_sem=recv_sems.at[number],
            device_id=device, device_id_type=MESH,
        )
        copy.start()
        started.append(copy)
        return copy

    def local(src, dst, number):
        copy = pltpu.make_async_copy(src, dst, local_sems.at[number])
        copy.start()
        return copy

    mate = (flip(r, 0)[0], s)
    options = []
    for bit in range(1, rep_bits):
        other, here = flip(r, bit)
        options.append((other, s, here))
    other, here = flip(s, 0)
    options.append((r, other, here))
    partners, bits = [], []
    for i in range(dims):
        a, b = options[i], options[(i + 1) % dims]
        partners.append(tuple(a[k] + core * (b[k] - a[k]) for k in range(2)))
        bits.append(a[2] + core * (b[2] - a[2]))
    z_peers = [None] + [(r, ((zi + d) % z_count) * 2 + x) for d in range(1, z_count)]
    tp_zi = [first + (head + d) % KV_HEADS for d in range(KV_HEADS)]
    tp_peers = [(r, tp_zi[d] * 2 + x) for d in range(KV_HEADS)]

    quarter = r % split
    fetch = local(master_ref.at[:, pl.ds(pl.multiple_of(quarter * sub, SUB), sub), :], stage_in, 0)

    barrier = pltpu.get_barrier_semaphore()
    everyone = n_rep * n_shard
    me = r * n_shard + s

    @pl.loop(1, everyone)
    def _(i):
        peer = (me + i) % everyone
        pl.semaphore_signal(
            barrier, inc=1, device_id=(peer // n_shard, peer % n_shard), device_id_type=MESH)

    shape = small.shape[1:]
    line = lax.broadcasted_iota(jnp.int32, shape, 0)
    lane = lax.broadcasted_iota(jnp.int32, shape, 1)
    hot, reward = jnp.zeros(shape, jnp.float32), jnp.zeros(shape, jnp.float32)
    for j in range(SEQ_DEV):
        hot = jnp.where((line == j) & (lane == group_ref[0, j]), 1.0, hot)
        reward = jnp.where(line == j, reward_ref[0, j], reward)
    small[0] = jnp.concatenate(
        [jnp.sum(hot, axis=0, keepdims=True), jnp.sum(hot * reward, axis=0, keepdims=True),
         jnp.sum(hot * (reward * reward), axis=0, keepdims=True),
         jnp.zeros((5, hot.shape[1]), jnp.float32)], axis=0)
    token_t[...] = jnp.zeros_like(token_t)
    terms = token_rows(seq_ref[...], mask_ref[...], new_ref[...], old_ref[...], ref_ref[...])
    for j, row in enumerate(terms):
        token_t[j:j + 1, :toks] = row
    tokens = jnp.transpose(token_t[...])[:toks]
    pl.semaphore_wait(barrier, everyone - 1)

    stat_copies = [send(small.at[0], small_in.at[d - 1], z_peers[d]) for d in range(1, z_count)]

    fetch.wait()
    for h in range(KV_HEADS):
        for l in range(layer_count):
            stage_out[h, l, :, :HEAD] = stage_in[l, :, h * HEAD:(h + 1) * HEAD].astype(jnp.bfloat16)
            low = KV_HEADS * HEAD + h * HEAD
            stage_out[h, l, :, HEAD:] = stage_in[l, :, low:low + HEAD].astype(jnp.bfloat16)
    yi = quarter // 2
    xy = [(r, flip(s, 0)[0])]
    first_at = (1 - x, yi)
    if split == 4:
        other = flip(r, 1)[0]
        xy = [(r + core * (other - r), s + (1 - core) * (1 - 2 * x)),
              (r + (1 - core) * (other - r), s + core * (1 - 2 * x))]
        first_at = (x + (1 - core) * (1 - 2 * x), yi + core * (1 - 2 * yi))
        second_at = (x + core * (1 - 2 * x), yi + (1 - core) * (1 - 2 * yi))
        third_at = (1 - x, 1 - yi)
    spread_copies = []

    def spread_block(d):
        for e in range(d, z_count if d == KV_HEADS - 1 else d + 1):
            if e:
                m1[e - 1].wait_recv()
            else:
                own_copy.wait()
            block = mb_ref.at[core, x, yi, (zi + z_count - e) % z_count]
            spread_copies.append([send(block, block, device) for device in xy])

    for copy in stat_copies:
        copy.wait_recv()
    slot = z_count - 1
    total = small[0]
    for d in range(1, z_count):
        total = total + small_in[d - 1]
    small[1] = total
    level = 1
    for k, device in enumerate([mate] + partners):
        copy = send(small.at[level], small_in.at[slot], device)
        if k == 0:
            own_copy = local(stage_out.at[head], mb_ref.at[core, x, yi, zi], 1)
            m1 = [send(stage_out.at[(head + d) % KV_HEADS], mb_ref.at[core, x, yi, zi], z_peers[d])
                  for d in range(1, z_count)]
        if k == 1:
            spread_block(0)
        copy.wait_recv()
        total = total + small_in[slot]
        slot += 1
        level += 1
        small[level] = total

    count = jnp.maximum(total[0:1], 1.0)
    mean = total[1:2] / count
    spread = jnp.maximum(jnp.sqrt(jnp.maximum(total[2:3] / count - mean * mean, 0.0)), 0.5)
    own_mean = jnp.sum(hot * mean, axis=1, keepdims=True)
    own_std = jnp.sum(hot * spread, axis=1, keepdims=True)
    own_std = jnp.where(own_std > 0.0, own_std, 1.0)
    advantage = (reward[:, 0:1] - own_mean) / own_std
    coef = tokens[:, SEQ_DEV:SEQ_DEV + 1]
    for j in range(SEQ_DEV):
        coef = coef + tokens[:, j:j + 1] * advantage[j:j + 1, :]
    for h in range(KV_HEADS):
        for side in range(2):
            low = side * KV_HEADS * HEAD + h * HEAD
            at = h * WIDE + side * HEAD
            delta[:, at:at + HEAD] = (coef * cot_ref[:, low:low + HEAD].astype(jnp.float32)).astype(jnp.bfloat16)

    spread_block(1)
    half = features // 2

    def multiply(base):
        @pl.loop(0, half // TILE)
        def _(i):
            at = pl.multiple_of(base + i * TILE, TILE)
            out = lax.dot_general(
                hidden_ref[:, pl.ds(at, TILE)], delta[...], (((0,), (0,)), ((), ())),
                preferred_element_type=jnp.float32,
            ).astype(jnp.bfloat16)
            for h in range(KV_HEADS):
                part[h, pl.ds(at, TILE), :] = out[:, h * WIDE:(h + 1) * WIDE]

    offsets, lens = [core * half], [half]
    for i in range(dims):
        lens.append(lens[-1] // 2)
        offsets.append(offsets[-1] + bits[i] * lens[-1])
    starts, at = [], 0
    for length in lens:
        starts.append(at)
        at += length
    order = [(head + k + 1) % KV_HEADS for k in range(KV_HEADS)]

    away = (1 - core) * half
    multiply(away)
    inbound = {}
    for k in range(KV_HEADS):
        inbound[0, k] = send(
            part.at[order[k], pl.ds(pl.multiple_of(away, SUB), half)],
            sums.at[order[k], pl.ds(starts[0], half)], mate)
    spread_block(2)
    multiply(core * half)

    spread_block(3)
    own_block = mb_ref.at[core, x, yi]
    to_mate = [send(own_block, own_block, mate)]
    forward = []

    inner = min(lens[-1], 112)

    def add_in(i, h):
        base = offsets[i]

        @pl.loop(0, lens[i] // inner)
        def _(t):
            at = pl.multiple_of(base + t * inner, SUB)
            from_at = pl.multiple_of(starts[i] + t * inner, SUB)
            part[h, pl.ds(at, inner), :] = (
                part[h, pl.ds(at, inner), :].astype(jnp.float32)
                + sums[h, pl.ds(from_at, inner), :].astype(jnp.float32)
            ).astype(jnp.bfloat16)

    z_copies = []
    for t in range(KV_HEADS + dims):
        for i in range(dims + 1):
            k = t - i
            if k < 0 or k >= KV_HEADS:
                continue
            inbound[i, k].wait_recv()
            add_in(i, order[k])
            if i < dims:
                gone = offsets[i] + (1 - bits[i]) * lens[i + 1]
                inbound[i + 1, k] = send(
                    part.at[order[k], pl.ds(pl.multiple_of(gone, SUB), lens[i + 1])],
                    sums.at[order[k], pl.ds(starts[i + 1], lens[i + 1])], partners[i])
            else:
                for d in range(1, z_count):
                    if d % KV_HEADS == (k + 1) % KV_HEADS:
                        z_copies.append(send(
                            part.at[order[k], pl.ds(pl.multiple_of(offsets[-1], SUB), lens[-1])],
                            zin.at[d - 1], z_peers[d]))
        if t == 3 and split == 4:
            for pair in spread_copies:
                pair[0].wait_recv()
            block = mb_ref.at[core, first_at[0], first_at[1]]
            forward.append(send(block, block, xy[1]))
            to_mate.append(send(block, block, mate))

    for copy in z_copies:
        copy.wait_recv()
    base = offsets[-1]

    def gather_sum(t, acc):
        at = pl.multiple_of(base + t * inner, SUB)
        g = part[head, pl.ds(at, inner), :].astype(jnp.float32)
        for d in range(1, z_count):
            g = g + zin[d - 1, pl.ds(pl.multiple_of(t * inner, SUB), inner), :].astype(jnp.float32)
        grad[pl.ds(at, inner), :] = g.astype(jnp.bfloat16)
        return acc + jnp.sum(g * g, axis=0, keepdims=True)

    squares = lax.fori_loop(0, lens[-1] // inner, gather_sum, jnp.zeros((1, WIDE), jnp.float32))
    square = jnp.broadcast_to(jnp.sum(squares, axis=1, keepdims=True), small.shape[1:])
    mine = pl.ds(pl.multiple_of(base, SUB), lens[-1])
    s_dst, inside = base // rows, base % rows
    pieces = rows // lens[-1]
    nm_number = counter[0]
    nm_in = nm_number + n_rep // 2
    counter[0] = nm_in + KV_HEADS * pieces
    nm_copies = [
        pltpu.make_async_remote_copy(
            src_ref=grad.at[mine], dst_ref=rows_in.at[head, pl.ds(pl.multiple_of(inside, SUB), lens[-1])],
            send_sem=send_sems.at[nm_number + j],
            recv_sem=recv_sems.at[nm_in + head * pieces + inside // lens[-1]],
            device_id=(2 * j + core, s_dst), device_id_type=MESH)
        for j in range(n_rep // 2)]
    dst_zi = s_dst // 2
    leaves = (dst_zi != zi) & (dst_zi // KV_HEADS == zi // KV_HEADS)
    level += 1
    small[level] = square
    square_copies = []
    for d in range(1, KV_HEADS):
        square_copies.append(send(small.at[level], small_in.at[slot], tp_peers[d]))
        slot += 1
    slot_base = slot - (KV_HEADS - 1)

    first_span = pl.ds(pl.multiple_of(offsets[dims], SUB), lens[dims])
    first_copy = send(grad.at[first_span], grad.at[first_span], partners[dims - 1])

    @pl.when(leaves)
    def _():
        for copy in nm_copies:
            copy.start()

    for step, i in enumerate(list(reversed(range(dims))) + [-1]):
        device = mate if i < 0 else partners[i]
        span = pl.ds(pl.multiple_of(offsets[i + 1], SUB), lens[i + 1])
        copy = first_copy if step == 0 else send(grad.at[span], grad.at[span], device)
        if step == 0:
            for other in square_copies:
                other.wait_recv()
            for d in range(KV_HEADS - 1):
                square = square + small_in[slot_base + d]
        level += 1
        small[level] = square
        square_copy = send(small.at[level], small_in.at[slot], device)
        square_copy.wait_recv()
        square = square + small_in[slot]
        slot += 1
        copy.wait_recv()

    if split == 4:
        for pair in spread_copies:
            pair[1].wait_recv()
        block = mb_ref.at[core, second_at[0], second_at[1]]
        to_mate.append(send(block, block, mate))
        forward[0].wait_recv()
        block = mb_ref.at[core, third_at[0], third_at[1]]
    else:
        for pair in spread_copies:
            pair[0].wait_recv()
        block = mb_ref.at[core, first_at[0], first_at[1]]
    to_mate.append(send(block, block, mate))

    rms = jnp.sqrt(square / (features * KV_HEADS * WIDE) + 1e-06)
    scale_ref[...] = 0.5 / rms[:, :LANES]
    done = [local(grad, gb_out, 0)]
    done.append(local(grad.at[pl.ds(pl.multiple_of(s * rows, SUB), rows)], nm_out.at[head], 1))
    others = [(head + d) % KV_HEADS for d in range(1, KV_HEADS)]
    pass_number = counter[0]
    counter[0] += KV_HEADS - 1
    passed = [
        pltpu.make_async_remote_copy(
            src_ref=rows_in.at[h], dst_ref=rows_in.at[h], send_sem=send_sems.at[pass_number + n],
            recv_sem=recv_sems.at[pass_number + n], device_id=mate, device_id_type=MESH)
        for n, h in enumerate(others)]
    keeper = (s * rows) // half

    @pl.when(core == keeper)
    def _():
        for n, h in enumerate(others):
            for p in range(pieces):
                pltpu.make_async_remote_copy(
                    src_ref=rows_in.at[h, pl.ds(p * lens[-1], lens[-1])],
                    dst_ref=rows_in.at[h, pl.ds(p * lens[-1], lens[-1])],
                    send_sem=send_sems.at[nm_number], recv_sem=recv_sems.at[nm_in + h * pieces + p],
                    device_id=mate, device_id_type=MESH).wait_recv()
            passed[n].start()

    @pl.when(core != keeper)
    def _():
        for copy in passed:
            copy.wait_recv()

    for n, h in enumerate(others):
        done.append(local(rows_in.at[h], nm_out.at[h], n + 2))
    for copy in to_mate:
        copy.wait_recv()

    @pl.when(core == keeper)
    def _():
        for copy in passed:
            copy.wait_send()

    @pl.when(leaves)
    def _():
        for copy in nm_copies:
            copy.wait_send()

    for copy in done:
        copy.wait()
    for copy in started:
        copy.wait_send()


def finish_kernel(mb_ref, gb_ref, nm_ref, scale_ref, master_ref, new_ref, out_ref):
    scale = scale_ref[0:1, 0:1]
    for h in range(KV_HEADS):
        for side in range(2):
            low = side * KV_HEADS * HEAD + h * HEAD
            new_ref[:, low:low + HEAD] = (
                master_ref[0, :, low:low + HEAD]
                - scale * nm_ref[h, :, side * HEAD:(side + 1) * HEAD].astype(jnp.float32))
    _, _, y_count, z_count, layer_count, sub, _ = mb_ref.shape
    for z in range(z_count):
        for x in range(2):
            for y in range(y_count):
                for c in range(2):
                    at = (((z * 2 + x) * y_count + y) * 2 + c) * sub
                    span = slice(at, at + sub)
                    out_ref[0, span, :] = (
                        mb_ref[c, x, y, z, 0].astype(jnp.float32)
                        - scale * gb_ref[span, :].astype(jnp.float32)).astype(jnp.bfloat16)
                    for l in range(1, layer_count):
                        out_ref[l, span, :] = mb_ref[c, x, y, z, l]


def per_device(
    n_rep, n_shard, hidden, cotangent, seq_ids, response_mask, group_ids, rewards, new_logp, old_logp, ref_logp,
    master,
):
    groups = n_rep * n_shard * SEQ_DEV // 8
    wide = -(-groups // LANES) * LANES
    toks, features = hidden.shape
    layer_count, rows, cols = master.shape
    z_count = n_shard // 2
    split = 4 if n_rep % 4 == 0 and (rows // 4) % SUB == 0 else 2
    sub = rows // split
    dims = n_rep.bit_length() - 1
    final = features // 2 ** (dims + 1)
    bf16, f32 = jnp.bfloat16, jnp.float32
    vmem, hbm = pl.BlockSpec(memory_space=pltpu.VMEM), pl.BlockSpec(memory_space=pl.ANY)
    smem = pl.BlockSpec(memory_space=pltpu.SMEM)
    mb_shape = (2, 2, split // 2, z_count, layer_count, sub, WIDE)
    sem_count = 64 + 8 * z_count
    landing = features // 2 * 2
    mb, gb, nm, scale = pl.pallas_call(
        functools.partial(exchange_kernel, n_rep, n_shard, split),
        out_shape=(
            jax.ShapeDtypeStruct(mb_shape, bf16),
            jax.ShapeDtypeStruct((features, WIDE), bf16),
            jax.ShapeDtypeStruct((KV_HEADS, rows, WIDE), bf16),
            jax.ShapeDtypeStruct((8, LANES), f32),
        ),
        in_specs=[smem] * 2 + [vmem] * 7 + [hbm],
        out_specs=(hbm, hbm, hbm, vmem),
        scratch_shapes=[
            pltpu.VMEM((KV_HEADS, features, WIDE), bf16),
            pltpu.VMEM((KV_HEADS, landing, WIDE), bf16),
            pltpu.VMEM((z_count - 1, final, WIDE), bf16),
            pltpu.VMEM((features, WIDE), bf16),
            pltpu.VMEM((KV_HEADS, rows, WIDE), bf16),
            pltpu.VMEM((toks, cols), bf16),
            pltpu.VMEM((layer_count, sub, cols), f32),
            pltpu.VMEM((KV_HEADS, layer_count, sub, WIDE), bf16),
            pltpu.VMEM((2 * dims + 6, 8, wide), f32),
            pltpu.VMEM((z_count + 2 * dims + 6, 8, wide), f32),
            pltpu.VMEM((LANES, -(-toks // LANES) * LANES), f32),
            pltpu.SemaphoreType.DMA((sem_count,)),
            pltpu.SemaphoreType.DMA((sem_count,)),
            pltpu.SemaphoreType.DMA((8,)),
        ],
        compiler_params=pltpu.CompilerParams(
            collective_id=0, has_side_effects=True, vmem_limit_bytes=56 * 2**20
        ),
        name="exchange",
    )(group_ids, rewards, seq_ids, response_mask, new_logp, old_logp, ref_logp, hidden, cotangent, master)
    steps = KV_HEADS
    new_master, rollout = pl.pallas_call(
        finish_kernel,
        grid=(steps,),
        out_shape=(
            jax.ShapeDtypeStruct((rows, cols), f32),
            jax.ShapeDtypeStruct((layer_count, features, WIDE), bf16),
        ),
        in_specs=[
            pl.BlockSpec((2, 2, split // 2, z_count // steps, layer_count, sub, WIDE),
                         lambda i: (0, 0, 0, i, 0, 0, 0)),
            pl.BlockSpec((features // steps, WIDE), lambda i: (i, 0)),
            pl.BlockSpec((KV_HEADS, rows // steps, WIDE), lambda i: (0, i, 0)),
            pl.BlockSpec((8, LANES), lambda i: (0, 0)),
            pl.BlockSpec((1, rows // steps, cols), lambda i: (0, i, 0)),
        ],
        out_specs=(
            pl.BlockSpec((rows // steps, cols), lambda i: (i, 0)),
            pl.BlockSpec((layer_count, features // steps, WIDE), lambda i: (0, i, 0)),
        ),
        name="finish",
    )(mb, gb, nm, scale, master)
    return (new_master, rollout)


def solution(mesh):
    tokens = P(("rep", "shard"), None)
    return jax.shard_map(
        functools.partial(per_device, mesh.shape["rep"], mesh.shape["shard"]),
        mesh=mesh,
        in_specs=(tokens,) * 9 + (P(None, "shard", None),),
        out_specs=(P("shard", None), P(None, None, "shard")),
        check_vma=False,
    )
```
